32 devices in a mesh: row: 2 (over x), col: 4 (over z), depth: 4 (over y, core).
Axes of the slice: x: 2, y: 2, z: 4, core: 2. Of those that a mesh axis runs over, the one named last changes fastest.
Arguments:
- spd_matrix: float32 [16384, 16384], P('row', ('col', 'depth')), may hold values from -8 to 24
Outputs:
- panel_factor: float32 [16384, 512], P('row')
- schur_part: float32 [16384, 16384], P('row', ('col', 'depth'))
The draws below stay inside these ranges and needn't reach their ends.
All inputs are finite; a program needn't handle non-finite values.
Results may differ from the reference program's by a relative error of at most 0.00015.
Values sent between devices are 32-bit elements; how exact they have to be, the bound alone decides.
A program may use at most 192 MiB of HBM per device.

```python
import math
import jax
import jax.numpy as jnp
from jax import lax

ORDER = 16384
PANEL = 512


def draw_spd_matrix(key, part):
    first = jax.random.fold_in(key, 11)
    second = jax.random.fold_in(key, 12)
    third = jax.random.fold_in(key, 13)
    loads = jnp.clip(jax.random.normal(first, (ORDER, PANEL), jnp.float32), -6.0, 6.0)
    noise = jnp.clip(jax.random.normal(second, (ORDER, ORDER), jnp.float32), -6.0, 6.0)
    diagonal = jax.random.uniform(third, (ORDER,), jnp.float32, 3.0, 5.0)
    loads = loads * math.sqrt(3.0 / PANEL)
    noise = noise * (0.5 / math.sqrt(ORDER))
    gram = jnp.dot(loads, loads.T, precision=lax.Precision.HIGHEST, preferred_element_type=jnp.float32)
    gram = (gram + gram.T) * 0.5
    return noise + noise.T + gram + jnp.diag(diagonal)


def setup_inputs(seed: int = 0) -> dict:
    arg_keys = jax.random.split(jax.random.key(seed), 2)
    spd_matrix = draw_spd_matrix(jax.random.fold_in(arg_keys[1], 71), 0)
    return {"spd_matrix": spd_matrix}


def reference(spd_matrix):
    pivot = spd_matrix[:PANEL, :PANEL]
    pivot_factor = jnp.linalg.cholesky(pivot)
    panel_factor = lax.linalg.triangular_solve(pivot_factor, spd_matrix[:, :PANEL], left_side=False, lower=True, transpose_a=True)
    update = lax.dot_general(panel_factor.astype(jnp.float32), panel_factor.astype(jnp.float32), (((1,), (1,)), ((), ())), precision=lax.Precision.HIGHEST, preferred_element_type=jnp.float32)
    return (panel_factor, spd_matrix - update)
```

```python
import functools

import jax
import jax.numpy as jnp
from jax import lax
from jax.experimental import pallas as pl
from jax.experimental.pallas import tpu as pltpu
from jax.sharding import PartitionSpec as P

PANEL = 512
NB = 128
PIECES = 8
MESH = pl.DeviceIdType.MESH
HIGHEST = lax.Precision.HIGHEST
CR = (((1,), (1,)), ((), ()))
CC = (((1,), (0,)), ((), ()))


def dot(a, b, dims=CC, precision=None):
    return lax.dot_general(a, b, dims, precision=precision, preferred_element_type=jnp.float32)


def split(x):
    hi = x.astype(jnp.bfloat16)
    return hi, (x - hi.astype(jnp.float32)).astype(jnp.bfloat16)


def dot3(a, b, dims=CC):
    (ah, al), (bh, bl) = a, b
    return dot(ah, bh, dims) + (dot(ah, bl, dims) + dot(al, bh, dims))


def block_inverse_factor(block):
    rows = lax.broadcasted_iota(jnp.int32, (NB, NB), 0)
    lanes = lax.broadcasted_iota(jnp.int32, (NB, NB), 1)
    a = block
    x = jnp.where(rows == lanes, 1.0, 0.0).astype(jnp.float32)
    sub = lax.broadcasted_iota(jnp.int32, (8, NB), 0)
    done = []
    for j in range(NB):
        r = j % 8
        row, xrow = a[r : r + 1, :], x[r : r + 1, :]
        s = lax.rsqrt(jnp.broadcast_to(row[:, j : j + 1], (1, NB)))
        row, xrow = row * s, xrow * s
        col = jnp.broadcast_to(a[:, j : j + 1], a.shape) * s
        head = jnp.where(sub > r, col[:8], 0.0)
        xhead = jnp.where(sub == r, xrow, x[:8] - head * xrow)
        if a.shape[0] > 8:
            tail = col[8:]
            xtail = x[8:] - tail * xrow
            atail = a[8:] - tail * row
            if r == 7:
                done.append(xhead)
                a, x = atail, xtail
            else:
                a = jnp.concatenate([a[:8] - head * row, atail], axis=0)
                x = jnp.concatenate([xhead, xtail], axis=0)
        else:
            a = a[:8] - head * row
            x = xhead
    done.append(x)
    return jnp.concatenate(done, axis=0)


def factor_kernel(pivot_ref, w_ref, a_ref):
    n = pivot_ref.shape[0]
    a_ref[...] = pivot_ref[...]
    rows = lax.broadcasted_iota(jnp.int32, (n, n), 0)
    lanes = lax.broadcasted_iota(jnp.int32, (n, n), 1)
    w_ref[...] = jnp.where(rows == lanes, 1.0, 0.0).astype(jnp.float32)
    below = lax.broadcasted_iota(jnp.int32, (n, NB), 0)

    @pl.loop(0, n // NB)
    def _(k):
        here = pl.ds(pl.multiple_of(k * NB, NB), NB)
        wkk = block_inverse_factor(a_ref[here, here])
        w_ref[here, :] = dot(wkk, w_ref[here, :], CC, HIGHEST)
        col = jnp.where(below >= (k + 1) * NB, a_ref[:, here], 0.0)
        col = dot(col, wkk, CR, HIGHEST)
        a_ref[...] -= dot(col, col, CR, HIGHEST)
        w_ref[...] -= dot(col, w_ref[here, :], CC, HIGHEST)


def inverse_factor(pivot):
    n = pivot.shape[0]
    return pl.pallas_call(
        factor_kernel,
        name="inverse_factor",
        out_shape=jax.ShapeDtypeStruct((n, n), jnp.float32),
        in_specs=[pl.BlockSpec(memory_space=pltpu.VMEM)],
        out_specs=pl.BlockSpec(memory_space=pltpu.VMEM),
        scratch_shapes=[pltpu.VMEM((n, n), jnp.float32)],
        cost_estimate=pl.CostEstimate(flops=60 * 10**9, bytes_accessed=2 * 4 * n * n, transcendentals=0),
    )(pivot)


def update_kernel(w_ref, top_ref, raw_ref, a_ref, panel_ref, out_ref, wh, wl, bh, bl):
    @pl.when(pl.program_id(0) == 0)
    def _():
        w = split(w_ref[...])
        wh[...], wl[...] = w
        bh[...], bl[...] = split(dot3(w, split(top_ref[...])))

    raw = split(raw_ref[0].T)
    panel = dot3(raw, (wh[...], wl[...]), CR)
    panel_ref[...] = panel
    out_ref[...] = a_ref[...] - dot3(split(panel), (bh[...], bl[...]))


def update(w, top, raw, a):
    chunks, n, width = raw.shape
    rows, cols = a.shape
    return pl.pallas_call(
        update_kernel,
        name="panel_and_update",
        grid=(chunks,),
        out_shape=(
            jax.ShapeDtypeStruct((rows, n), jnp.float32),
            jax.ShapeDtypeStruct((rows, cols), jnp.float32),
        ),
        in_specs=[
            pl.BlockSpec((n, n), lambda i: (0, 0)),
            pl.BlockSpec((n, cols), lambda i: (0, 0)),
            pl.BlockSpec((1, n, width), lambda i: (i, 0, 0)),
            pl.BlockSpec((width, cols), lambda i: (i, 0)),
        ],
        out_specs=(
            pl.BlockSpec((width, n), lambda i: (i, 0)),
            pl.BlockSpec((width, cols), lambda i: (i, 0)),
        ),
        scratch_shapes=[
            pltpu.VMEM((n, n), jnp.bfloat16),
            pltpu.VMEM((n, n), jnp.bfloat16),
            pltpu.VMEM((n, cols), jnp.bfloat16),
            pltpu.VMEM((n, cols), jnp.bfloat16),
        ],
        compiler_params=pltpu.CompilerParams(vmem_limit_bytes=50 * 2**20),
    )(w, top, raw, a)


def spread_kernel(groups, cols, depths, a_ref, out_ref, held, load_sem, send_sem, recv_sem, store_sem):
    n = held.shape[1] * PIECES
    size = n // PIECES
    r, c, d = lax.axis_index("row"), lax.axis_index("col"), lax.axis_index("depth")
    even = lax.rem(d, 2) == 0
    trunk = (c == 0) & even
    root = (r == 0) & (c == 0) & (d == 0)
    children = (
        ((r, lax.min(c + 1, cols - 1), d), even & (c < cols - 1)),
        ((r, c, lax.min(d + 2, depths - 1)), trunk & (d < depths - 2)),
        ((lax.min(r + 1, groups - 1), c, d), trunk & (d == 0) & (r < groups - 1)),
        ((r, c, lax.min(d + 1, depths - 1)), even),
    )
    parents = (
        ((r, lax.max(c - 1, 0), d), even & (c > 0)),
        ((r, c, lax.max(d - 2, 0)), trunk & (d > 0)),
        ((lax.max(r - 1, 0), c, d), trunk & (d == 0) & (r > 0)),
        ((r, c, lax.max(d - 1, 0)), lax.rem(d, 2) == 1),
    )
    barrier = pltpu.get_barrier_semaphore()
    for device, there in children + parents:

        @pl.when(there)
        def _(device=device):
            pl.semaphore_signal(barrier, inc=1, device_id=device, device_id_type=MESH)

    peers = sum(jnp.where(there, 1, 0) for _, there in children + parents)
    pl.semaphore_wait(barrier, peers)

    def load(p):
        return pltpu.make_async_copy(
            a_ref.at[pl.ds(p * size, size), pl.ds(0, n)], held.at[p], load_sem.at[p]
        )

    def send(p, k):
        return pltpu.make_async_remote_copy(
            src_ref=held.at[p],
            dst_ref=held.at[p],
            send_sem=send_sem.at[p, k],
            recv_sem=recv_sem.at[p],
            device_id=children[k][0],
            device_id_type=MESH,
        )

    def store(p):
        return pltpu.make_async_copy(held.at[p], out_ref.at[pl.ds(p * size, size)], store_sem.at[p])

    @pl.when(root)
    def _():
        for p in range(PIECES):
            load(p).start()

    for p in range(PIECES):

        @pl.when(root)
        def _():
            load(p).wait()

        @pl.when(jnp.logical_not(root))
        def _():
            send(p, 0).wait_recv()

        for k in range(4):

            @pl.when(children[k][1])
            def _():
                send(p, k).start()

        store(p).start()
    for p in range(PIECES):
        for k in range(4):

            @pl.when(children[k][1])
            def _():
                send(p, k).wait_send()

        store(p).wait()


def spread_pivot(groups, cols, depths, spd_matrix):
    n = PANEL
    return pl.pallas_call(
        functools.partial(spread_kernel, groups, cols, depths),
        name="spread_pivot",
        out_shape=jax.ShapeDtypeStruct((n, n), jnp.float32),
        in_specs=[pl.BlockSpec(memory_space=pl.ANY)],
        out_specs=pl.BlockSpec(memory_space=pl.ANY),
        scratch_shapes=[
            pltpu.VMEM((PIECES, n // PIECES, n), jnp.float32),
            pltpu.SemaphoreType.DMA((PIECES,)),
            pltpu.SemaphoreType.DMA((PIECES, 4)),
            pltpu.SemaphoreType.DMA((PIECES,)),
            pltpu.SemaphoreType.DMA((PIECES,)),
        ],
        compiler_params=pltpu.CompilerParams(collective_id=0, has_side_effects=True),
        cost_estimate=pl.CostEstimate(flops=10**10, bytes_accessed=8 * n * n, transcendentals=0),
    )(spd_matrix)


def shards(groups, colsplit, depths, spd_matrix):
    blocks = colsplit * depths
    axes = ("row", "col", "depth")
    cols = spd_matrix.shape[1]
    width = cols // groups
    row = lax.axis_index("row")
    place = row * blocks + lax.axis_index(("col", "depth"))
    mine = spd_matrix[:PANEL, :]

    pivot = spread_pivot(groups, colsplit, depths, spd_matrix)

    arrived = []
    for h in range(groups):
        pairs = [(q // groups, q) for q in range(h, groups * blocks, groups)]
        arrived.append(lax.ppermute(mine[:, h * width : (h + 1) * width], axes, pairs))
    arrived, pivot = lax.optimization_barrier((arrived, pivot))
    piece = arrived[0]
    for h in range(1, groups):
        piece = jnp.where(lax.rem(place, groups) == h, arrived[h], piece)
    piece, mine = lax.optimization_barrier((piece, mine))
    raw = lax.all_gather(piece, ("col", "depth"), axis=0, tiled=False)

    if groups == 2:
        got = lax.ppermute(mine, "row", [(0, 1)])
        top = jnp.where(row == 0, mine, got)
    else:
        top = lax.psum(jnp.where(row == 0, mine, 0.0), "row")

    w = inverse_factor(pivot)
    return update(w, top, raw, spd_matrix)


def solution(mesh):
    groups = mesh.shape["row"]
    placed = (P("row", ("col", "depth")),)
    return jax.shard_map(
        functools.partial(shards, groups, mesh.shape["col"], mesh.shape["depth"]),
        mesh=mesh,
        in_specs=placed,
        out_specs=(P("row", None), P("row", ("col", "depth"))),
        check_vma=False,
    )
```

```python
import functools

import jax
import jax.numpy as jnp
from jax import lax
from jax.experimental import pallas as pl
from jax.experimental.pallas import tpu as pltpu
from jax.sharding import PartitionSpec as P

PANEL = 512
NB = 128
PIECES = 8
MESH = pl.DeviceIdType.MESH
HIGHEST = lax.Precision.HIGHEST
CR = (((1,), (1,)), ((), ()))
CC = (((1,), (0,)), ((), ()))


def dot(a, b, dims=CC, precision=None):
    return lax.dot_general(a, b, dims, precision=precision, preferred_element_type=jnp.float32)


def split(x):
    hi = x.astype(jnp.bfloat16)
    return hi, (x - hi.astype(jnp.float32)).astype(jnp.bfloat16)


def dot3(a, b, dims=CC):
    (ah, al), (bh, bl) = a, b
    return dot(ah, bh, dims) + (dot(ah, bl, dims) + dot(al, bh, dims))


def block_inverse_factor(block):
    rows = lax.broadcasted_iota(jnp.int32, (NB, NB), 0)
    lanes = lax.broadcasted_iota(jnp.int32, (NB, NB), 1)
    a = block
    x = jnp.where(rows == lanes, 1.0, 0.0).astype(jnp.float32)
    sub = lax.broadcasted_iota(jnp.int32, (8, NB), 0)
    done = []
    for j in range(NB):
        r = j % 8
        row, xrow = a[r : r + 1, :], x[r : r + 1, :]
        s = lax.rsqrt(jnp.broadcast_to(row[:, j : j + 1], (1, NB)))
        row, xrow = row * s, xrow * s
        col = jnp.broadcast_to(a[:, j : j + 1], a.shape) * s
        head = jnp.where(sub > r, col[:8], 0.0)
        xhead = jnp.where(sub == r, xrow, x[:8] - head * xrow)
        if a.shape[0] > 8:
            tail = col[8:]
            xtail = x[8:] - tail * xrow
            atail = a[8:] - tail * row
            if r == 7:
                done.append(xhead)
                a, x = atail, xtail
            else:
                a = jnp.concatenate([a[:8] - head * row, atail], axis=0)
                x = jnp.concatenate([xhead, xtail], axis=0)
        else:
            a = a[:8] - head * row
            x = xhead
    done.append(x)
    return jnp.concatenate(done, axis=0)


def factor_kernel(pivot_ref, w_ref, a_ref):
    n = pivot_ref.shape[0]
    a_ref[...] = pivot_ref[...]
    rows = lax.broadcasted_iota(jnp.int32, (n, n), 0)
    lanes = lax.broadcasted_iota(jnp.int32, (n, n), 1)
    w_ref[...] = jnp.where(rows == lanes, 1.0, 0.0).astype(jnp.float32)
    below = lax.broadcasted_iota(jnp.int32, (n, NB), 0)

    @pl.loop(0, n // NB)
    def _(k):
        here = pl.ds(pl.multiple_of(k * NB, NB), NB)
        wkk = block_inverse_factor(a_ref[here, here])
        w_ref[here, :] = dot(wkk, w_ref[here, :], CC, HIGHEST)
        col = jnp.where(below >= (k + 1) * NB, a_ref[:, here], 0.0)
        col = dot(col, wkk, CR, HIGHEST)
        a_ref[...] -= dot(col, col, CR, HIGHEST)
        w_ref[...] -= dot(col, w_ref[here, :], CC, HIGHEST)


def inverse_factor(pivot):
    n = pivot.shape[0]
    return pl.pallas_call(
        factor_kernel,
        name="inverse_factor",
        out_shape=jax.ShapeDtypeStruct((n, n), jnp.float32),
        in_specs=[pl.BlockSpec(memory_space=pltpu.VMEM)],
        out_specs=pl.BlockSpec(memory_space=pltpu.VMEM),
        scratch_shapes=[pltpu.VMEM((n, n), jnp.float32)],
        cost_estimate=pl.CostEstimate(flops=60 * 10**9, bytes_accessed=2 * 4 * n * n, transcendentals=0),
    )(pivot)


def update_kernel(w_ref, top_ref, raw_ref, a_ref, panel_ref, out_ref, wh, wl, bh, bl):
    @pl.when(pl.program_id(0) == 0)
    def _():
        w = split(w_ref[...])
        wh[...], wl[...] = w
        bh[...], bl[...] = split(dot3(w, split(top_ref[...])))

    raw = split(raw_ref[0].T)
    half = wh.shape[0] // 2
    panel = jnp.concatenate(
        [
            dot3([p[:, :half] for p in raw], (wh[:half, :half], wl[:half, :half]), CR),
            dot3(raw, (wh[half:, :], wl[half:, :]), CR),
        ],
        axis=1,
    )
    panel_ref[...] = panel
    out_ref[...] = a_ref[...] - dot3(split(panel), (bh[...], bl[...]))


def update(w, top, raw, a):
    chunks, n, width = raw.shape
    rows, cols = a.shape
    return pl.pallas_call(
        update_kernel,
        name="panel_and_update",
        grid=(chunks,),
        out_shape=(
            jax.ShapeDtypeStruct((rows, n), jnp.float32),
            jax.ShapeDtypeStruct((rows, cols), jnp.float32),
        ),
        in_specs=[
            pl.BlockSpec((n, n), lambda i: (0, 0)),
            pl.BlockSpec((n, cols), lambda i: (0, 0)),
            pl.BlockSpec((1, n, width), lambda i: (i, 0, 0)),
            pl.BlockSpec((width, cols), lambda i: (i, 0)),
        ],
        out_specs=(
            pl.BlockSpec((width, n), lambda i: (i, 0)),
            pl.BlockSpec((width, cols), lambda i: (i, 0)),
        ),
        scratch_shapes=[
            pltpu.VMEM((n, n), jnp.bfloat16),
            pltpu.VMEM((n, n), jnp.bfloat16),
            pltpu.VMEM((n, cols), jnp.bfloat16),
            pltpu.VMEM((n, cols), jnp.bfloat16),
        ],
        compiler_params=pltpu.CompilerParams(vmem_limit_bytes=50 * 2**20),
    )(w, top, raw, a)


def spread_kernel(groups, cols, depths, a_ref, out_ref, held, load_sem, send_sem, recv_sem, store_sem):
    n = held.shape[1] * PIECES
    size = n // PIECES
    r, c, d = lax.axis_index("row"), lax.axis_index("col"), lax.axis_index("depth")
    even = lax.rem(d, 2) == 0
    trunk = (c == 0) & even
    root = (r == 0) & (c == 0) & (d == 0)
    children = (
        ((r, lax.min(c + 1, cols - 1), d), even & (c < cols - 1)),
        ((r, c, lax.min(d + 2, depths - 1)), trunk & (d < depths - 2)),
        ((lax.min(r + 1, groups - 1), c, d), trunk & (d == 0) & (r < groups - 1)),
        ((r, c, lax.min(d + 1, depths - 1)), even),
    )
    parents = (
        ((r, lax.max(c - 1, 0), d), even & (c > 0)),
        ((r, c, lax.max(d - 2, 0)), trunk & (d > 0)),
        ((lax.max(r - 1, 0), c, d), trunk & (d == 0) & (r > 0)),
        ((r, c, lax.max(d - 1, 0)), lax.rem(d, 2) == 1),
    )
    barrier = pltpu.get_barrier_semaphore()
    for device, there in children + parents:

        @pl.when(there)
        def _(device=device):
            pl.semaphore_signal(barrier, inc=1, device_id=device, device_id_type=MESH)

    peers = sum(jnp.where(there, 1, 0) for _, there in children + parents)
    pl.semaphore_wait(barrier, peers)

    def load(p):
        return pltpu.make_async_copy(
            a_ref.at[pl.ds(p * size, size), pl.ds(0, n)], held.at[p], load_sem.at[p]
        )

    def send(p, k):
        return pltpu.make_async_remote_copy(
            src_ref=held.at[p],
            dst_ref=held.at[p],
            send_sem=send_sem.at[p, k],
            recv_sem=recv_sem.at[p],
            device_id=children[k][0],
            device_id_type=MESH,
        )

    def store(p):
        return pltpu.make_async_copy(held.at[p], out_ref.at[pl.ds(p * size, size)], store_sem.at[p])

    @pl.when(root)
    def _():
        for p in range(PIECES):
            load(p).start()

    for p in range(PIECES):

        @pl.when(root)
        def _():
            load(p).wait()

        @pl.when(jnp.logical_not(root))
        def _():
            send(p, 0).wait_recv()

        for k in range(4):

            @pl.when(children[k][1])
            def _():
                send(p, k).start()

        store(p).start()
    for p in range(PIECES):
        for k in range(4):

            @pl.when(children[k][1])
            def _():
                send(p, k).wait_send()

        store(p).wait()


def spread_pivot(groups, cols, depths, spd_matrix):
    n = PANEL
    return pl.pallas_call(
        functools.partial(spread_kernel, groups, cols, depths),
        name="spread_pivot",
        out_shape=jax.ShapeDtypeStruct((n, n), jnp.float32),
        in_specs=[pl.BlockSpec(memory_space=pl.ANY)],
        out_specs=pl.BlockSpec(memory_space=pl.ANY),
        scratch_shapes=[
            pltpu.VMEM((PIECES, n // PIECES, n), jnp.float32),
            pltpu.SemaphoreType.DMA((PIECES,)),
            pltpu.SemaphoreType.DMA((PIECES, 4)),
            pltpu.SemaphoreType.DMA((PIECES,)),
            pltpu.SemaphoreType.DMA((PIECES,)),
        ],
        compiler_params=pltpu.CompilerParams(collective_id=0, has_side_effects=True),
        cost_estimate=pl.CostEstimate(flops=10**10, bytes_accessed=8 * n * n, transcendentals=0),
    )(spd_matrix)


def shards(groups, colsplit, depths, spd_matrix):
    blocks = colsplit * depths
    axes = ("row", "col", "depth")
    cols = spd_matrix.shape[1]
    width = cols // groups
    row = lax.axis_index("row")
    place = row * blocks + lax.axis_index(("col", "depth"))
    mine = spd_matrix[:PANEL, :]

    pivot = spread_pivot(groups, colsplit, depths, spd_matrix)

    arrived = []
    for h in range(groups):
        pairs = [(q // groups, q) for q in range(h, groups * blocks, groups)]
        arrived.append(lax.ppermute(mine[:, h * width : (h + 1) * width], axes, pairs))
    arrived, pivot = lax.optimization_barrier((arrived, pivot))
    piece = arrived[0]
    for h in range(1, groups):
        piece = jnp.where(lax.rem(place, groups) == h, arrived[h], piece)
    piece, mine = lax.optimization_barrier((piece, mine))
    raw = lax.all_gather(piece, ("col", "depth"), axis=0, tiled=False)

    if groups == 2:
        got = lax.ppermute(mine, "row", [(0, 1)])
        top = jnp.where(row == 0, mine, got)
    else:
        top = lax.psum(jnp.where(row == 0, mine, 0.0), "row")

    w = inverse_factor(pivot)
    return update(w, top, raw, spd_matrix)


def solution(mesh):
    groups = mesh.shape["row"]
    placed = (P("row", ("col", "depth")),)
    return jax.shard_map(
        functools.partial(shards, groups, mesh.shape["col"], mesh.shape["depth"]),
        mesh=mesh,
        in_specs=placed,
        out_specs=(P("row", None), P("row", ("col", "depth"))),
        check_vma=False,
    )
```
